8 devices in a mesh: rep: 2 (over y, z), dp: 4 (over x, core).
Axes of the slice: x: 2, y: 2, z: 1, core: 2. Of those that a mesh axis runs over, the one named last changes fastest.
Arguments:
- x: bfloat16 [8, 2048, 1536], P(('rep', 'dp')), parts along dimension 0
- dy: bfloat16 [8, 2048, 1536], P(('rep', 'dp')), parts along dimension 0
- w_gate: bfloat16 [2, 1536, 3584], replicated
- w_up: bfloat16 [2, 1536, 3584], replicated
- w_down: bfloat16 [2, 3584, 1536], replicated
- m_w_gate: float32 [2, 1536, 3584], replicated
- m_w_up: float32 [2, 1536, 3584], replicated
- m_w_down: float32 [2, 3584, 1536], replicated
- v_w_gate: float32 [2, 1536, 3584], replicated
- v_w_up: float32 [2, 1536, 3584], replicated
- v_w_down: float32 [2, 3584, 1536], replicated
Outputs:
- output 1: bfloat16 [4, 1536, 3584], P('rep'), parts along dimension 0
- output 2: bfloat16 [4, 1536, 3584], P('rep'), parts along dimension 0
- output 3: bfloat16 [4, 3584, 1536], P('rep'), parts along dimension 0
- output 4: float32 [4, 1536, 3584], P('rep'), parts along dimension 0
- output 5: float32 [4, 1536, 3584], P('rep'), parts along dimension 0
- output 6: float32 [4, 3584, 1536], P('rep'), parts along dimension 0
- output 7: float32 [4, 1536, 3584], P('rep'), parts along dimension 0
- output 8: float32 [4, 1536, 3584], P('rep'), parts along dimension 0
- output 9: float32 [4, 3584, 1536], P('rep'), parts along dimension 0
There are 2 independent parts. The reference program is written for one: setup_inputs(seed, part) draws one part's arguments, and reference() takes and returns one part's arrays. A program takes and returns all parts, laid end to end along the dimension named above; an argument that names none is the same for every part.
All inputs are finite; a program needn't handle non-finite values.
Results may differ from the reference program's by a relative error of at most 0.02.
Values are sent between devices in bfloat16 or wider.
A program may use at most 3 GiB of HBM per device.

```python
import jax
import jax.numpy as jnp
from jax import lax

SEQUENCES = 4
TOKENS = 2048
D = 1536
FF = 3584
LAYERS = 2
NAMES = ("w_gate", "w_up", "w_down")
SHAPES = {"w_gate": (LAYERS, D, FF), "w_up": (LAYERS, D, FF), "w_down": (LAYERS, FF, D)}


def bump(key, n, height):
    away = (jnp.arange(n, dtype=jnp.int32) - jax.random.randint(key, (), 0, n, jnp.int32)) % n
    return jnp.where(away < n // 8, height, 1.0)


def together(key, own, strength):
    shared = jax.random.normal(key, own.shape[1:], jnp.float32)
    return (own + strength * shared) * lax.rsqrt(1 + strength * strength)


def setup_inputs(seed: int = 0, part: int = 0) -> dict:
    kx, kdy, ka, kb, kz, kf, kh, kl, *keys = jax.random.split(jax.random.key(seed), 8 + 3 * len(NAMES))
    kx, kdy, ka, kb = (jax.random.fold_in(k, part) for k in (kx, kdy, ka, kb))
    kw, km, kv = (keys[i::3] for i in range(3))
    shape = (SEQUENCES, TOKENS, D)
    much_x, much_dy = jax.random.uniform(kz, (2,), jnp.float32, 0.0, 1.0)
    loud = 2.0 ** jax.random.uniform(jax.random.fold_in(kz, 1), (), jnp.float32, -1.0, 2.0)
    layers = 2.0 ** jax.random.uniform(kl, (LAYERS, 1, 1), jnp.float32, -1.0, 1.0)
    x = together(ka, jax.random.normal(kx, shape, jnp.float32), much_x) * bump(kf, D, 4.0)
    dy = together(kb, jax.random.normal(kdy, shape, jnp.float32), much_dy)
    drawn = {"x": x.astype(jnp.bfloat16), "dy": (loud * dy * (SEQUENCES * TOKENS) ** -0.5).astype(jnp.bfloat16)}
    for key, name in zip(kw, NAMES, strict=True):
        w = jax.random.normal(key, SHAPES[name], jnp.float32) * SHAPES[name][1] ** -0.5
        drawn[name] = (w * {"w_gate": 1.0, "w_up": bump(kh, FF, 4.0), "w_down": layers}[name]).astype(jnp.bfloat16)
    for key, name in zip(km, NAMES, strict=True):
        drawn[f"m_{name}"] = 0.1 * jax.random.normal(key, SHAPES[name], jnp.float32)
    for key, name in zip(kv, NAMES, strict=True):
        drawn[f"v_{name}"] = jax.random.uniform(key, SHAPES[name], jnp.float32, 0.005, 0.015)
    return drawn


def matmul(a, w):
    return jnp.dot(a, w, preferred_element_type=jnp.float32).astype(jnp.bfloat16)


def normed(h):
    wide = h.astype(jnp.float32)
    scale = lax.rsqrt(jnp.mean(wide**2, -1, keepdims=True) + 1e-6)
    return (wide * scale).astype(jnp.bfloat16)


def layer(h, w):
    a = normed(h)
    gate = jnp.dot(a, w["w_gate"], preferred_element_type=jnp.float32)
    up = jnp.dot(a, w["w_up"], preferred_element_type=jnp.float32)
    return h + matmul((jax.nn.silu(gate) * up).astype(jnp.bfloat16), w["w_down"])


def adamw(w, m, v, g):
    m = 0.9 * m + 0.1 * g
    v = 0.95 * v + 0.05 * g * g
    step = m * lax.rsqrt(v + 1e-8) + 0.1 * w
    return (w - 0.02 * step).astype(jnp.bfloat16), m, v


def stack(weights, h):
    return lax.scan(lambda h, w: (layer(h, w), None), h, weights)[0]


def reference(x, dy, w_gate, w_up, w_down, m_w_gate, m_w_up, m_w_down, v_w_gate, v_w_up, v_w_down):
    weights = dict(zip(NAMES, (w_gate, w_up, w_down), strict=True))

    def take(so_far, sequence):
        h, by_y = sequence
        _, back = jax.vjp(lambda w: stack(w, h), weights)
        return jax.tree.map(lambda total, term: total + term.astype(jnp.float32), so_far, back(by_y)[0]), None

    none_yet = {name: jnp.zeros(w.shape, jnp.float32) for name, w in weights.items()}
    by_weights, _ = lax.scan(take, none_yet, (x, dy))
    gradients = [by_weights[name].astype(jnp.bfloat16).astype(jnp.float32) for name in NAMES]
    new = [
        adamw(w.astype(jnp.float32), m, v, g)
        for w, m, v, g in zip((w_gate, w_up, w_down), (m_w_gate, m_w_up, m_w_down), (v_w_gate, v_w_up, v_w_down), gradients, strict=True)
    ]
    return tuple(one[which] for which in range(3) for one in new)
```

```python
import jax
import jax.numpy as jnp
from jax import lax
from jax.experimental import pallas as pl
from jax.experimental.pallas import tpu as pltpu
from jax.sharding import PartitionSpec as P


F32, BF16 = jnp.float32, jnp.bfloat16
PARTNER = [(0, 1), (1, 0), (2, 3), (3, 2)]
ACROSS = [(0, 2), (2, 0), (1, 3), (3, 1)]


def dot(a, b, dims):
    return lax.dot_general(a, b, (dims, ((), ())), preferred_element_type=F32)


def scale_of(h):
    wide = h.astype(F32)
    return lax.rsqrt(jnp.mean(wide**2, -1, keepdims=True) + 1e-6)


def normed(h):
    return (h.astype(F32) * scale_of(h)).astype(BF16)


def adamw_kernel(side, g, w, m, v, *refs):
    new_w, new_m, new_v = refs[-3:]
    g = g[...].astype(F32)[None]
    one = 0.9 * m[...] + 0.1 * g
    two = 0.95 * v[...] + 0.05 * g * g
    step = one * lax.rsqrt(two + 1e-8) + 0.1 * w[...].astype(F32)
    new_w[...] = (w[...].astype(F32) - 0.02 * step).astype(BF16)
    new_m[...] = one
    new_v[...] = two


def adamw(side, g, w, m, v, layer, by_rows, so_far):
    rows, cols = g.shape
    tile = 96 if by_rows else 256
    steps = rows // tile
    if by_rows:
        where = lambda i, s: (layer, s[0] * steps + i, 0)
    else:
        where = lambda i, s: (layer, i, s[0])
    block = pl.BlockSpec((1, tile, cols), where)
    kept = [] if so_far is None else list(so_far)
    return pl.pallas_call(
        adamw_kernel,
        grid_spec=pltpu.PrefetchScalarGridSpec(
            num_scalar_prefetch=1,
            grid=(steps,),
            in_specs=[pl.BlockSpec((tile, cols), lambda i, s: (i, 0)), block, block, block] + [pl.BlockSpec(memory_space=pl.ANY)] * len(kept),
            out_specs=[block] * 3,
        ),
        out_shape=[jax.ShapeDtypeStruct(w.shape, BF16), jax.ShapeDtypeStruct(w.shape, F32), jax.ShapeDtypeStruct(w.shape, F32)],
        input_output_aliases={5 + i: i for i in range(len(kept))},
        cost_estimate=pl.CostEstimate(flops=rows * cols * 4000, bytes_accessed=rows * cols * 22, transcendentals=rows * cols),
        name="adamw",
    )(side, g, w, m, v, *kept)


def solution(mesh):
    def step(x, dy, *arrays):
        weights, m, v = (arrays[i : i + 3] for i in (0, 3, 6))
        layers = weights[0].shape[0]
        h, dy = x[0], dy[0]
        half = h.shape[-1] // 2
        me = lax.axis_index("dp") % 2
        mine, others = me.astype(jnp.int32)[None], (1 - me).astype(jnp.int32)[None]
        w_gate, w_up, w_down = ([w[n] for n in range(layers)] for w in weights)
        kept = []
        for n in range(layers):
            a = normed(h)
            gate, up = (dot(a, w[n], ((1,), (0,))) for w in (w_gate, w_up))
            hidden = (jax.nn.silu(gate) * up).astype(BF16)
            kept.append((h, a, gate, up, hidden))
            if n < layers - 1:
                h = h + dot(hidden, w_down[n], ((1,), (0,))).astype(BF16)

        def after(x, *others):
            return lax.optimization_barrier((x, *others))[0]

        waiting = []

        def reduce(which, layer, thin, wide):
            by_rows = which < 2

            def term(piece):
                return (dot(piece, wide, ((0,), (0,))) if by_rows else dot(wide, piece, ((0,), (0,)))).astype(BF16)

            theirs, ours = (lax.dynamic_slice(thin, (0, side * half), (thin.shape[0], half)) for side in (1 - me, me))
            first = lax.optimization_barrier(term(theirs))
            got = lax.ppermute(first, "dp", PARTNER)
            second = term(after(ours, first))
            own = lax.optimization_barrier((second.astype(F32) + got.astype(F32)).astype(BF16))
            far = lax.ppermute(own, "dp", ACROSS)
            waiting.append((which, layer, own, far))
            return own

        by = dy
        for n in reversed(range(layers)):
            h, a, gate, up, hidden = kept[n]
            done = reduce(2, n, by, hidden)
            by_hidden = dot(after(by, done), w_down[n], ((1,), (1,))).astype(BF16).astype(F32)
            sig = jax.nn.sigmoid(gate)
            by_up = (by_hidden * (gate * sig)).astype(BF16)
            by_gate = (by_hidden * up * (sig * (1 + gate * (1 - sig)))).astype(BF16)
            a, by_up, by_gate = lax.optimization_barrier((a, by_up, by_gate))
            done = reduce(1, n, a, by_up)
            done = reduce(0, n, after(a, done), by_gate)
            if n:
                by_a = dot(after(by_gate, done), w_gate[n], ((1,), (1,))).astype(BF16).astype(F32)
                by_a = (by_a + dot(by_up, w_up[n], ((1,), (1,))).astype(BF16).astype(F32)).astype(BF16).astype(F32)
                wide, scale = h.astype(F32), scale_of(h)
                inner = jnp.sum(by_a * wide, -1, keepdims=True) / wide.shape[-1]
                by = by + (scale * by_a - wide * (scale**3 * inner)).astype(BF16)

        new = [None] * 3
        for which, layer, own, far in waiting:
            far = after(far, done)
            total = lax.optimization_barrier((own.astype(F32) + far.astype(F32)).astype(BF16))
            other = lax.ppermute(total, "dp", PARTNER)
            new[which] = adamw(mine, total, weights[which], m[which], v[which], layer, which < 2, new[which])
            new[which] = adamw(others, other, weights[which], m[which], v[which], layer, which < 2, new[which])
            done = new[which][0]
        return tuple(new[i][which] for which in range(3) for i in range(3))

    return jax.shard_map(
        step,
        mesh=mesh,
        in_specs=(P(("rep", "dp"), None, None),) * 2 + (P(None, None, None),) * 9,
        out_specs=(P("rep", None, None),) * 9,
        check_vma=False,
    )
```

```python
import functools

import jax
import jax.numpy as jnp
from jax import lax
from jax.experimental import pallas as pl
from jax.experimental.pallas import tpu as pltpu
from jax.sharding import PartitionSpec as P


F32, BF16 = jnp.float32, jnp.bfloat16
PARTNER = [(0, 1), (1, 0), (2, 3), (3, 2)]
ACROSS = [(0, 2), (2, 0), (1, 3), (3, 1)]
GATE, UP, DOWN = range(3)
TILE = 256
ROWS = {"forward": 1024, "turn": 1024, "back": 2048}
MIB = {"forward": 62, "turn": 62, "back": 62, "term": 62, "adamw": 62}
ANY = pl.BlockSpec(memory_space=pl.ANY)


def dot(a, b, dims):
    return lax.dot_general(a, b, (dims, ((), ())), preferred_element_type=F32)


def fixed(shape, where=None):
    return pl.BlockSpec(shape, where or (lambda j, s: (0,) * len(shape)), pipeline_mode=pl.Buffered(1))


def cost(flops, moved):
    return pl.CostEstimate(flops=int(flops), bytes_accessed=int(moved), transcendentals=0)


def norm_into(h_ref, a_ref):
    @pl.when(pl.program_id(0) == 0)
    def _():
        @pl.loop(0, h_ref.shape[0], step=TILE)
        def _(r):
            wide = h_ref[pl.ds(r, TILE), :].astype(F32)
            scale = lax.rsqrt(jnp.mean(wide * wide, -1, keepdims=True) + 1e-6)
            a_ref[pl.ds(r, TILE), :] = (wide * scale).astype(BF16)


def forward_kernel(_, h, w_gate, w_up, a, hidden, gate, up):
    norm_into(h, a)
    for r in range(0, h.shape[0], ROWS["forward"]):
        rows = slice(r, r + ROWS["forward"])
        g, u = dot(a[rows], w_gate[0], ((1,), (0,))), dot(a[rows], w_up[0], ((1,), (0,)))
        gate[rows], up[rows] = g, u
        hidden[rows] = (g * jax.nn.sigmoid(g) * u).astype(BF16)


def backward(by_hidden, g, u):
    by_hidden = by_hidden.astype(BF16).astype(F32)
    sig = jax.nn.sigmoid(g)
    silu = g * sig
    return (by_hidden * u * (sig + silu * (1 - sig))).astype(BF16), (by_hidden * silu).astype(BF16), (silu * u).astype(BF16)


def turn_kernel(_, h, by, w_gate, w_up, w_down, a, hidden, by_gate, by_up):
    norm_into(h, a)
    for r in range(0, h.shape[0], ROWS["turn"]):
        rows = slice(r, r + ROWS["turn"])
        g, u = dot(a[rows], w_gate[0], ((1,), (0,))), dot(a[rows], w_up[0], ((1,), (0,)))
        by_gate[rows], by_up[rows], hidden[rows] = backward(dot(by[rows], w_down[0], ((1,), (1,))), g, u)


def back_kernel(_, by, w_down, gate, up, by_gate, by_up):
    for r in range(0, by.shape[0], ROWS["back"]):
        rows = slice(r, r + ROWS["back"])
        by_gate[rows], by_up[rows], _ = backward(dot(by[rows], w_down[0], ((1,), (1,))), gate[rows], up[rows])


def call(kernel, name, scalars, tiles, ins, args, outs, shapes, flops, aliases={}):
    moved = sum(x.size * x.dtype.itemsize for x in shapes)
    return pl.pallas_call(
        kernel,
        grid_spec=pltpu.PrefetchScalarGridSpec(num_scalar_prefetch=1, grid=(tiles,), in_specs=ins, out_specs=outs),
        out_shape=shapes,
        input_output_aliases=aliases,
        cost_estimate=cost(flops, moved),
        compiler_params=pltpu.CompilerParams(vmem_limit_bytes=MIB[name] << 20),
    )(scalars, *args)


def weight_in(layer, d):
    return pl.BlockSpec((1, d, TILE), lambda j, s: (layer, 0, s[0] + j))


def weight_out(layer, d):
    return pl.BlockSpec((1, TILE, d), lambda j, s: (layer, s[0] + j, 0))


def shaped(*shape, dtype=BF16):
    return jax.ShapeDtypeStruct(shape, dtype)


def forward(h, w, layer, start):
    t, d = h.shape
    f = w[GATE].shape[-1]
    column = pl.BlockSpec((t, TILE), lambda j, s: (0, j))
    return call(
        forward_kernel, "forward", start, f // TILE,
        [fixed((t, d)), weight_in(layer, d), weight_in(layer, d)], (h, w[GATE], w[UP]),
        [fixed((t, d)), column, column, column],
        [shaped(t, d), shaped(t, f), shaped(t, f, dtype=F32), shaped(t, f, dtype=F32)], 4 * t * d * f,
    )


def turn(h, by, w, layer, start, f):
    t, d = h.shape
    column = pl.BlockSpec((t, TILE), lambda j, s: (0, j))
    return call(
        turn_kernel, "turn", start, f // TILE,
        [fixed((t, d)), fixed((t, d)), weight_in(layer, d), weight_in(layer, d), weight_out(layer, d)], (h, by, *w),
        [fixed((t, d)), column, column, column], [shaped(t, d)] + [shaped(t, f)] * 3, 6 * t * d * f,
    )


def back(by, w, gate, up, layer, start):
    t, d = by.shape
    f = gate.shape[-1]
    column = pl.BlockSpec((t, TILE), lambda j, s: (0, j))
    return call(
        back_kernel, "back", start, f // TILE, [fixed((t, d)), weight_out(layer, d), column, column], (by, w[DOWN], gate, up),
        [column, column], [shaped(t, f)] * 2, 2 * t * d * f,
    )


def term_kernel(pairs, added, _, *refs):
    ins, out = refs[:-1], refs[-1]
    total = None
    for n in range(pairs):
        part = dot(ins[2 * n][...], ins[2 * n + 1][...], ((0,), (0,)))
        total = part if total is None else total + part
    if added:
        total = total + ins[-1][...].astype(F32)
    out[...] = total.astype(BF16)


def term(where, pairs, m, n, tile, got=None, old=None, layer=None):
    t = pairs[0][0].shape[0]
    ins, args = [], []
    for i, (left, right) in enumerate(pairs):
        ins.append(fixed((t, m), functools.partial(lambda i, j, s: (0, s[i]), i)))
        ins.append(pl.BlockSpec((t, tile), functools.partial(lambda i, j, s: (0, s[i] + j), len(pairs) + i)))
        args += [left, right]
    out = pl.BlockSpec((m, tile), lambda j, s: (0, j))
    if got is not None:
        ins.append(out)
        args.append(got)
    scalars = jnp.stack([jnp.asarray(x, jnp.int32) for x in where])
    if old is not None:
        block = pl.BlockSpec((1, m, tile), lambda j, s: (layer, s[2 * len(pairs)], s[2 * len(pairs) + 1] + j))
        return call(
            functools.partial(last_term_kernel, len(pairs)), "term", scalars, n // tile, ins + [block] * 3, args + list(old), [out] + [block] * 3,
            [shaped(m, n)] + [shaped(*x.shape, dtype=x.dtype) for x in old], 2 * t * m * n * len(pairs),
        )
    return call(
        functools.partial(term_kernel, len(pairs), got is not None), "term", scalars, n // tile, ins, args, [out], [shaped(m, n)], 2 * t * m * n * len(pairs),
    )[0]


def stepped(g, w, m, v, new_w, new_m, new_v):
    one = 0.9 * m[0] + 0.1 * g
    two = 0.95 * v[0] + 0.05 * g * g
    wide = w[0].astype(F32)
    new_w[0] = (wide - 0.02 * (one * lax.rsqrt(two + 1e-8) + 0.1 * wide)).astype(BF16)
    new_m[0] = one
    new_v[0] = two


def last_term_kernel(pairs, _, *refs):
    total = refs[2 * pairs][...].astype(F32)
    for n in range(pairs):
        total = total + dot(refs[2 * n][...], refs[2 * n + 1][...], ((0,), (0,)))
    total = total.astype(BF16)
    refs[-4][...] = total
    stepped(total.astype(F32), *refs[2 * pairs + 1 : 2 * pairs + 4], *refs[-3:])


def adamw_kernel(terms, steps, s, *refs):
    w, m, v = refs[2 * terms : 2 * terms + 3] if steps else refs[terms : terms + 3]
    new_w, new_m, new_v = refs[-3:]

    def block(gs):
        g = gs[0][...].astype(F32)
        if terms == 2:
            g = (g + gs[1][...].astype(F32)).astype(BF16).astype(F32)
        stepped(g, w, m, v, new_w, new_m, new_v)

    if steps:
        pl.when(pl.program_id(0) < steps)(lambda: block(refs[:terms]))
        pl.when(pl.program_id(0) >= steps)(lambda: block(refs[terms : 2 * terms]))
    else:
        block(refs[:terms])


def adamw(terms, where, old, layer, tile, so_far, others=()):
    rows, cols = terms[0].shape
    steps = rows // tile

    def place(i, s):
        if not others:
            return (layer, s[0] * steps + i, s[1])
        later = (i >= steps).astype(jnp.int32)
        return (layer, jnp.where(later == 1, s[2] * steps + i - steps, s[0] * steps + i), jnp.where(later == 1, s[3], s[1]))

    block = pl.BlockSpec((1, tile, cols), place)
    g = [pl.BlockSpec((tile, cols), lambda i, s: (jnp.minimum(i, steps - 1), 0))] * len(terms)
    g += [pl.BlockSpec((tile, cols), lambda i, s: (jnp.maximum(i - steps, 0), 0))] * len(others)
    kept = list(so_far or ())
    scalars = jnp.stack([jnp.asarray(x, jnp.int32) for x in where])
    return call(
        functools.partial(adamw_kernel, len(terms), steps if others else 0), "adamw", scalars, steps * (2 if others else 1),
        g + [block] * 3 + [ANY] * len(kept), (*terms, *others, *old, *kept),
        [block] * 3, [shaped(*x.shape, dtype=x.dtype) for x in old], rows * cols * 4000, {len(g) + 4 + i: i for i in range(len(kept))},
    )


def after(x, *others):
    return lax.optimization_barrier((x, *others))[0]


def solution(mesh):
    def step(x, dy, *arrays):
        w, m, v = (arrays[i : i + 3] for i in (0, 3, 6))
        old = list(zip(w, m, v))
        h0, by1 = x[0], dy[0]
        _, d = h0.shape
        f = w[GATE].shape[-1]
        me = lax.axis_index("dp") % 2
        chip = lax.axis_index("dp") // 2
        sides = ((1 - me), me)
        zero = jnp.zeros((1,), jnp.int32)
        share, base = f // 2, chip * (f // 2 // TILE)

        def across(x):
            return lax.ppermute(x, "dp", ACROSS)

        def partner(x):
            return lax.ppermute(x, "dp", PARTNER)

        barrier = lax.optimization_barrier

        far_by1 = across(by1)
        a0, hidden0, gate0, up0 = forward(h0, w, 0, zero)
        h1 = barrier(h0 + dot(hidden0, w[DOWN][0], ((1,), (0,))).astype(BF16))
        far_h1 = across(h1)
        a1, hidden1, by_gate1, by_up1 = barrier(turn(h1, by1, w, 1, zero, f))
        by_a = dot(by_gate1, w[GATE][1], ((1,), (1,))).astype(BF16).astype(F32) + dot(by_up1, w[UP][1], ((1,), (1,))).astype(BF16).astype(F32)
        by_a, wide = by_a.astype(BF16).astype(F32), h1.astype(F32)
        scale = lax.rsqrt(jnp.mean(wide**2, -1, keepdims=True) + 1e-6)
        inner = jnp.sum(by_a * wide, -1, keepdims=True) / d
        by0 = barrier(by1 + (scale * by_a - wide * (scale**3 * inner)).astype(BF16))

        def left0(side, pair, size, tile, got=None):
            return term((side, 0), [pair], size, pair[1].shape[1], tile, got)

        sums, far, near = {}, {}, {}
        piece = f // 4
        theirs = [barrier(left0(sides[0] * 2, (hidden0, by0), piece, TILE))]
        got = [partner(theirs[0])]
        theirs.append(barrier(left0(sides[0] * 2 + 1, (after(hidden0, theirs[0]), by0), piece, TILE)))
        got.append(partner(theirs[1]))
        sums[DOWN] = [barrier(left0(sides[1] * 2, (after(hidden0, theirs[1]), by0), piece, TILE, got[0]))]
        far[DOWN] = [across(sums[DOWN][0])]
        near[DOWN] = [partner(sums[DOWN][0])]
        sums[DOWN].append(barrier(left0(sides[1] * 2 + 1, (after(hidden0, sums[DOWN][0]), by0), piece, TILE, got[1])))
        far[DOWN].append(across(sums[DOWN][1]))
        near[DOWN].append(partner(sums[DOWN][1]))
        by_gate0, by_up0 = barrier(back(after(by0, sums[DOWN][1]), w, gate0, up0, 0, zero))
        up_theirs = barrier(left0(sides[0], (a0, by_up0), d // 2, 512))
        up_got = partner(up_theirs)
        gate_theirs = barrier(left0(sides[0], (after(a0, up_theirs), by_gate0), d // 2, 512))
        gate_got = partner(gate_theirs)
        sums[UP] = barrier(left0(sides[1], (after(a0, gate_theirs), by_up0), d // 2, 512, up_got))
        far[UP] = across(sums[UP])
        near[UP] = partner(sums[UP])
        sums[GATE] = barrier(left0(sides[1], (after(a0, sums[UP]), by_gate0), d // 2, 512, gate_got))
        far[GATE] = across(sums[GATE])
        near[GATE] = partner(sums[GATE])

        far_h1, far_by1 = barrier((far_h1, far_by1, sums[GATE]))[:2]
        far_a1, far_hidden1, far_by_gate1, far_by_up1 = barrier(turn(far_h1, far_by1, w, 1, base[None].astype(jnp.int32), share))

        def left1(side, which, got=None, behind=None):
            if which == DOWN:
                pairs = [(hidden1, by1), (far_hidden1, far_by1)]
                places, size, n, tile = (chip * 2 + side, side, 0, 0), share // 2, d, TILE
            else:
                pairs = [(a1, (by_gate1, by_up1)[which]), (far_a1, (far_by_gate1, far_by_up1)[which])]
                places, size, n, tile = (side, side, base, 0), d // 2, share, TILE
            if behind is not None:
                pairs[0] = (after(pairs[0][0], behind), pairs[0][1])
            if got is None:
                return barrier(term(places, pairs, size, n, tile))
            corner = (chip * 2 + side, 0) if which == DOWN else (side, base)
            total, *new[which] = barrier(term(places + corner, pairs, size, n, tile, got, old[which], 1))
            return total

        new, theirs, own1 = [None] * 3, {}, {}
        theirs[DOWN] = left1(sides[0], DOWN)
        got = partner(theirs[DOWN])
        theirs[UP] = left1(sides[0], UP, None, theirs[DOWN])
        got_up = partner(theirs[UP])
        own1[DOWN] = left1(sides[1], DOWN, got, theirs[UP])
        far1 = {DOWN: across(own1[DOWN])}
        near1 = {DOWN: partner(own1[DOWN])}
        theirs[GATE] = left1(sides[0], GATE, None, own1[DOWN])
        got_gate = partner(theirs[GATE])
        own1[UP] = left1(sides[1], UP, got_up, theirs[GATE])
        far1[UP] = across(own1[UP])
        near1[UP] = partner(own1[UP])
        own1[GATE] = left1(sides[1], GATE, got_gate, own1[UP])
        far1[GATE] = across(own1[GATE])
        near1[GATE] = partner(own1[GATE])

        last = own1[GATE]

        def optimize(which, layer, terms, where, tile, others=()):
            nonlocal last
            both = barrier((*terms, *others, last))
            terms, others = both[: len(terms)], both[len(terms) : -1]
            new[which] = adamw(terms, where, old[which], layer, tile, new[which], others)
            last = new[which][0]

        arrived = {}

        def beside(which):
            here = after(far1[which], last)
            arrived[which] = (here, partner(here))

        def first_layer(which):
            if which == DOWN:
                here = list(barrier((*far[which], last))[:2])
                places = [(side * 2, 0, side * 2 + 1, 0) for side in (me, 1 - me)]
                optimize(which, 0, (sums[which][0], here[0]), places[0], 224, (sums[which][1], here[1]))
                there = [partner(here[n]) for n in range(2)]
                optimize(which, 0, (near[which][0], there[0]), places[1], 224, (near[which][1], there[1]))
                return
            here = after(far[which], last)
            optimize(which, 0, (sums[which], here), (me, 0), 192)
            there = partner(here)
            if which == GATE:
                beside(DOWN)
            optimize(which, 0, (near[which], there), (1 - me, 0), 192)

        def places(which, of_chip):
            return [(of_chip * 2 + side, 0) if which == DOWN else (side, of_chip) for side in (me, 1 - me)]

        first_layer(DOWN)
        for which in (DOWN, UP, GATE):
            optimize(which, 1, (near1[which],), places(which, chip)[1], 224 if which == DOWN else 192)
        first_layer(UP)
        first_layer(GATE)
        for which in (DOWN, UP):
            if which == DOWN:
                beside(UP)
            (here, there), (first, second) = arrived[which], places(which, 1 - chip)
            optimize(which, 1, (here,), first + second, 224 if which == DOWN else 192, (there,))
        first, second = places(GATE, 1 - chip)
        here = after(far1[GATE], last)
        optimize(GATE, 1, (here,), first, 192)
        optimize(GATE, 1, (partner(here),), second, 192)
        return tuple(new[i][which] for which in range(3) for i in range(3))

    mapped = jax.shard_map(
        step,
        mesh=mesh,
        in_specs=(P(("rep", "dp"), None, None),) * 2 + (P(None, None, None),) * 9,
        out_specs=(P("rep", None, None),) * 9,
        check_vma=False,
    )

    def traced(*args):
        shapes = [jax.ShapeDtypeStruct(x.shape, x.dtype) for x in args]
        jax.eval_shape(mapped, *shapes)
        return mapped(*args)

    return traced
```

```python
import functools

import jax
import jax.numpy as jnp
from jax import lax
from jax.experimental import pallas as pl
from jax.experimental.pallas import tpu as pltpu
from jax.sharding import PartitionSpec as P


F32, BF16 = jnp.float32, jnp.bfloat16
PARTNER = [(0, 1), (1, 0), (2, 3), (3, 2)]
ACROSS = [(0, 2), (2, 0), (1, 3), (3, 1)]
GATE, UP, DOWN = range(3)
TILE = 256
ROWS = {"forward": 1024, "turn": 1024, "back": 2048}
MIB = {"forward": 62, "turn": 62, "back": 62, "term": 62, "adamw": 62}
ANY = pl.BlockSpec(memory_space=pl.ANY)


def dot(a, b, dims):
    return lax.dot_general(a, b, (dims, ((), ())), preferred_element_type=F32)


def fixed(shape, where=None):
    return pl.BlockSpec(shape, where or (lambda j, s: (0,) * len(shape)), pipeline_mode=pl.Buffered(1))


def cost(flops, moved):
    return pl.CostEstimate(flops=int(flops), bytes_accessed=int(moved), transcendentals=0)


def norm_into(h_ref, a_ref):
    @pl.when(pl.program_id(0) == 0)
    def _():
        @pl.loop(0, h_ref.shape[0], step=TILE)
        def _(r):
            wide = h_ref[pl.ds(r, TILE), :].astype(F32)
            scale = lax.rsqrt(jnp.mean(wide * wide, -1, keepdims=True) + 1e-6)
            a_ref[pl.ds(r, TILE), :] = (wide * scale).astype(BF16)


def forward_kernel(_, h, w_gate, w_up, a, hidden, gate, up):
    norm_into(h, a)
    for r in range(0, h.shape[0], ROWS["forward"]):
        rows = slice(r, r + ROWS["forward"])
        g, u = dot(a[rows], w_gate[0], ((1,), (0,))), dot(a[rows], w_up[0], ((1,), (0,)))
        gate[rows], up[rows] = g, u
        hidden[rows] = (g * jax.nn.sigmoid(g) * u).astype(BF16)


def backward(by_hidden, g, u):
    by_hidden = by_hidden.astype(BF16).astype(F32)
    sig = jax.nn.sigmoid(g)
    silu = g * sig
    return (by_hidden * u * (sig + silu * (1 - sig))).astype(BF16), (by_hidden * silu).astype(BF16), (silu * u).astype(BF16)


def turn_kernel(_, h, by, w_gate, w_up, w_down, a, hidden, by_gate, by_up):
    norm_into(h, a)
    for r in range(0, h.shape[0], ROWS["turn"]):
        rows = slice(r, r + ROWS["turn"])
        g, u = dot(a[rows], w_gate[0], ((1,), (0,))), dot(a[rows], w_up[0], ((1,), (0,)))
        by_gate[rows], by_up[rows], hidden[rows] = backward(dot(by[rows], w_down[0], ((1,), (1,))), g, u)


def back_kernel(_, by, w_down, gate, up, by_gate, by_up):
    for r in range(0, by.shape[0], ROWS["back"]):
        rows = slice(r, r + ROWS["back"])
        by_gate[rows], by_up[rows], _ = backward(dot(by[rows], w_down[0], ((1,), (1,))), gate[rows], up[rows])


def call(kernel, name, scalars, tiles, ins, args, outs, shapes, flops, aliases={}, scratch=()):
    moved = sum(x.size * x.dtype.itemsize for x in shapes)
    return pl.pallas_call(
        kernel,
        grid_spec=pltpu.PrefetchScalarGridSpec(num_scalar_prefetch=1, grid=(tiles,), in_specs=ins, out_specs=outs, scratch_shapes=scratch),
        out_shape=shapes,
        input_output_aliases=aliases,
        cost_estimate=cost(flops, moved),
        compiler_params=pltpu.CompilerParams(vmem_limit_bytes=MIB[name] << 20),
    )(scalars, *args)


def weight_in(layer, d):
    return pl.BlockSpec((1, d, TILE), lambda j, s: (layer, 0, s[0] + j))


def weight_out(layer, d):
    return pl.BlockSpec((1, TILE, d), lambda j, s: (layer, s[0] + j, 0))


def shaped(*shape, dtype=BF16):
    return jax.ShapeDtypeStruct(shape, dtype)


def forward(h, w, layer, start):
    t, d = h.shape
    f = w[GATE].shape[-1]
    column = pl.BlockSpec((t, TILE), lambda j, s: (0, j))
    return call(
        forward_kernel, "forward", start, f // TILE,
        [fixed((t, d)), weight_in(layer, d), weight_in(layer, d)], (h, w[GATE], w[UP]),
        [fixed((t, d)), column, column, column],
        [shaped(t, d), shaped(t, f), shaped(t, f, dtype=F32), shaped(t, f, dtype=F32)], 4 * t * d * f,
    )


def turn(h, by, w, layer, start, f):
    t, d = h.shape
    column = pl.BlockSpec((t, TILE), lambda j, s: (0, j))
    return call(
        turn_kernel, "turn", start, f // TILE,
        [fixed((t, d)), fixed((t, d)), weight_in(layer, d), weight_in(layer, d), weight_out(layer, d)], (h, by, *w),
        [fixed((t, d)), column, column, column], [shaped(t, d)] + [shaped(t, f)] * 3, 6 * t * d * f,
    )


def back(by, w, gate, up, layer, start):
    t, d = by.shape
    f = gate.shape[-1]
    column = pl.BlockSpec((t, TILE), lambda j, s: (0, j))
    return call(
        back_kernel, "back", start, f // TILE, [fixed((t, d)), weight_out(layer, d), column, column], (by, w[DOWN], gate, up),
        [column, column], [shaped(t, f)] * 2, 2 * t * d * f,
    )


def term_kernel(pairs, added, _, *refs):
    ins, out = refs[:-1], refs[-1]
    total = None
    for n in range(pairs):
        part = dot(ins[2 * n][...], ins[2 * n + 1][...], ((0,), (0,)))
        total = part if total is None else total + part
    if added:
        total = total + ins[-1][...].astype(F32)
    out[...] = total.astype(BF16)


def term(where, pairs, m, n, tile, got=None, old=None, layer=None, so_far=None, beside=None):
    t = pairs[0][0].shape[0]
    ins, args = [], []
    for i, (left, right) in enumerate(pairs):
        ins.append(fixed((t, m), functools.partial(lambda i, j, s: (0, s[i]), i)))
        ins.append(pl.BlockSpec((t, tile), functools.partial(lambda i, j, s: (0, s[i] + j), len(pairs) + i)))
        args += [left, right]
    out = pl.BlockSpec((m, tile), lambda j, s: (0, j))
    if got is not None:
        ins.append(out)
        args.append(got)
    scalars = jnp.stack([jnp.asarray(x, jnp.int32) for x in where])
    kept = list(so_far or ())
    if old is not None:
        block = pl.BlockSpec((1, m, tile), lambda j, s: (layer, s[2 * len(pairs)], s[2 * len(pairs) + 1] + j))
        return call(
            functools.partial(last_term_kernel, len(pairs)), "term", scalars, n // tile, ins + [block] * 3 + [ANY] * len(kept), args + list(old) + kept,
            [out] + [block] * 3, [shaped(m, n)] + [shaped(*x.shape, dtype=x.dtype) for x in old], 2 * t * m * n * len(pairs),
            {2 * len(pairs) + 5 + i: 1 + i for i in range(len(kept))},
        )
    if beside is not None:
        terms, old, layer = beside
        rows, cols = terms[0].shape
        rows //= n // tile
        block = pl.BlockSpec((1, rows, cols), lambda j, s: (layer, s[2 * len(pairs)] * (n // tile) + j, 0))
        return call(
            functools.partial(beside_kernel, len(pairs)), "term", scalars, n // tile,
            ins + [pl.BlockSpec((rows, cols), lambda j, s: (j, 0))] * 2 + [block] * 3 + [ANY] * len(kept), args + list(terms) + list(old) + kept,
            [out] + [block] * 3, [shaped(m, n)] + [shaped(*x.shape, dtype=x.dtype) for x in old], 2 * t * m * n * len(pairs),
            {2 * len(pairs) + 6 + i: 1 + i for i in range(len(kept))},
        )
    return call(
        functools.partial(term_kernel, len(pairs), got is not None), "term", scalars, n // tile, ins, args, [out], [shaped(m, n)], 2 * t * m * n * len(pairs),
    )[0]


def stepped(g, w, m, v, new_w, new_m, new_v, rows=slice(None)):
    one = 0.9 * m[0, rows] + 0.1 * g
    two = 0.95 * v[0, rows] + 0.05 * g * g
    wide = w[0, rows].astype(F32)
    new_w[0, rows] = (wide - 0.02 * (one * lax.rsqrt(two + 1e-8) + 0.1 * wide)).astype(BF16)
    new_m[0, rows] = one
    new_v[0, rows] = two


def last_term_kernel(pairs, _, *refs):
    total = refs[2 * pairs][...].astype(F32)
    for n in range(pairs):
        total = total + dot(refs[2 * n][...], refs[2 * n + 1][...], ((0,), (0,)))
    total = total.astype(BF16)
    refs[-4][...] = total
    stepped(total.astype(F32), *refs[2 * pairs + 1 : 2 * pairs + 4], *refs[-3:])


def beside_kernel(pairs, _, *refs):
    total = None
    for n in range(pairs):
        part = dot(refs[2 * n][...], refs[2 * n + 1][...], ((0,), (0,)))
        total = part if total is None else total + part
    refs[-4][...] = total.astype(BF16)
    g = (refs[2 * pairs][...].astype(F32) + refs[2 * pairs + 1][...].astype(F32)).astype(BF16).astype(F32)
    stepped(g, *refs[2 * pairs + 2 : 2 * pairs + 5], *refs[-3:])


def adamw_kernel(terms, steps, s, *refs):
    w, m, v = refs[2 * terms : 2 * terms + 3] if steps else refs[terms : terms + 3]
    new_w, new_m, new_v = refs[-3:]

    def block(gs):
        @pl.loop(0, gs[0].shape[0], step=32)
        def _(r):
            rows = pl.ds(r, 32)
            g = gs[0][rows].astype(F32)
            if terms == 2:
                g = (g + gs[1][rows].astype(F32)).astype(BF16).astype(F32)
            stepped(g, w, m, v, new_w, new_m, new_v, rows)

    if steps:
        pl.when(pl.program_id(0) < steps)(lambda: block(refs[:terms]))
        pl.when(pl.program_id(0) >= steps)(lambda: block(refs[terms : 2 * terms]))
    else:
        block(refs[:terms])


def adamw(terms, where, old, layer, tile, so_far, others=()):
    rows, cols = terms[0].shape
    steps = rows // tile

    def place(i, s):
        if not others:
            return (layer, s[0] * steps + i, s[1])
        later = (i >= steps).astype(jnp.int32)
        return (layer, jnp.where(later == 1, s[2] * steps + i - steps, s[0] * steps + i), jnp.where(later == 1, s[3], s[1]))

    block = pl.BlockSpec((1, tile, cols), place)
    g = [pl.BlockSpec((tile, cols), lambda i, s: (jnp.minimum(i, steps - 1), 0))] * len(terms)
    g += [pl.BlockSpec((tile, cols), lambda i, s: (jnp.maximum(i - steps, 0), 0))] * len(others)
    kept = list(so_far or ())
    scalars = jnp.stack([jnp.asarray(x, jnp.int32) for x in where])
    return call(
        functools.partial(adamw_kernel, len(terms), steps if others else 0), "adamw", scalars, steps * (2 if others else 1),
        g + [block] * 3 + [ANY] * len(kept), (*terms, *others, *old, *kept),
        [block] * 3, [shaped(*x.shape, dtype=x.dtype) for x in old], rows * cols * 4000, {len(g) + 4 + i: i for i in range(len(kept))},
    )


def after(x, *others):
    return lax.optimization_barrier((x, *others))[0]


def solution(mesh):
    def step(x, dy, *arrays):
        w, m, v = (arrays[i : i + 3] for i in (0, 3, 6))
        old = list(zip(w, m, v))
        h0, by1 = x[0], dy[0]
        _, d = h0.shape
        f = w[GATE].shape[-1]
        me = lax.axis_index("dp") % 2
        chip = lax.axis_index("dp") // 2
        sides = ((1 - me), me)
        zero = jnp.zeros((1,), jnp.int32)
        share, base = f // 2, chip * (f // 2 // TILE)

        def across(x):
            return lax.ppermute(x, "dp", ACROSS)

        def partner(x):
            return lax.ppermute(x, "dp", PARTNER)

        barrier = lax.optimization_barrier

        far_by1 = across(by1)
        a0, hidden0, gate0, up0 = forward(h0, w, 0, zero)
        h1 = barrier(h0 + dot(hidden0, w[DOWN][0], ((1,), (0,))).astype(BF16))
        far_h1 = across(h1)
        a1, hidden1, by_gate1, by_up1 = barrier(turn(h1, by1, w, 1, zero, f))
        by_a = dot(by_gate1, w[GATE][1], ((1,), (1,))).astype(BF16).astype(F32) + dot(by_up1, w[UP][1], ((1,), (1,))).astype(BF16).astype(F32)
        by_a, wide = by_a.astype(BF16).astype(F32), h1.astype(F32)
        scale = lax.rsqrt(jnp.mean(wide**2, -1, keepdims=True) + 1e-6)
        inner = jnp.sum(by_a * wide, -1, keepdims=True) / d
        by0 = barrier(by1 + (scale * by_a - wide * (scale**3 * inner)).astype(BF16))

        def left0(side, pair, size, tile, got=None):
            return term((side, 0), [pair], size, pair[1].shape[1], tile, got)

        sums, far, near = {}, {}, {}
        piece = f // 4
        theirs = [barrier(left0(sides[0] * 2, (hidden0, by0), piece, TILE))]
        got = [partner(theirs[0])]
        theirs.append(barrier(left0(sides[0] * 2 + 1, (after(hidden0, theirs[0]), by0), piece, TILE)))
        got.append(partner(theirs[1]))
        sums[DOWN] = [barrier(left0(sides[1] * 2, (after(hidden0, theirs[1]), by0), piece, TILE, got[0]))]
        far[DOWN] = [across(sums[DOWN][0])]
        near[DOWN] = [partner(sums[DOWN][0])]
        sums[DOWN].append(barrier(left0(sides[1] * 2 + 1, (after(hidden0, sums[DOWN][0]), by0), piece, TILE, got[1])))
        far[DOWN].append(across(sums[DOWN][1]))
        near[DOWN].append(partner(sums[DOWN][1]))
        by_gate0, by_up0 = barrier(back(after(by0, sums[DOWN][1]), w, gate0, up0, 0, zero))
        up_theirs = barrier(left0(sides[0], (a0, by_up0), d // 2, 512))
        up_got = partner(up_theirs)
        gate_theirs = barrier(left0(sides[0], (after(a0, up_theirs), by_gate0), d // 2, 512))
        gate_got = partner(gate_theirs)
        sums[UP] = barrier(left0(sides[1], (after(a0, gate_theirs), by_up0), d // 2, 512, up_got))
        far[UP] = across(sums[UP])
        near[UP] = partner(sums[UP])
        sums[GATE] = barrier(left0(sides[1], (after(a0, sums[UP]), by_gate0), d // 2, 512, gate_got))
        far[GATE] = across(sums[GATE])
        near[GATE] = partner(sums[GATE])

        far_h1, far_by1 = barrier((far_h1, far_by1, sums[GATE]))[:2]
        far_a1, far_hidden1, far_by_gate1, far_by_up1 = barrier(turn(far_h1, far_by1, w, 1, base[None].astype(jnp.int32), share))

        def left1(side, which, got=None, behind=None, piece=None):
            if which == DOWN:
                pairs = [(hidden1, by1), (far_hidden1, far_by1)]
                places, size, n, tile = (chip * 2 + side, side, 0, 0), share // 2, d, TILE
            else:
                pairs = [(a1, (by_gate1, by_up1)[which]), (far_a1, (far_by_gate1, far_by_up1)[which])]
                places, size, n, tile = (side, side, base, 0), d // 2, share, TILE
            if behind is not None:
                pairs[0] = (after(pairs[0][0], behind), pairs[0][1])
            if piece is not None:
                here = after(far[DOWN][piece], behind)
                passed[piece] = partner(here)
                terms = (sums[DOWN][piece], here)
                total, *new[DOWN] = barrier(term((*places, me * 2 + piece), pairs, size, n, tile, so_far=new[DOWN], beside=(terms, old[DOWN], 0)))
                return total
            if got is None:
                return barrier(term(places, pairs, size, n, tile))
            corner = (chip * 2 + side, 0) if which == DOWN else (side, base)
            total, *new[which] = barrier(term(places + corner, pairs, size, n, tile, got, old[which], 1, new[which]))
            return total

        new, theirs, own1, passed = [None] * 3, {}, {}, {}
        theirs[DOWN] = left1(sides[0], DOWN)
        got = partner(theirs[DOWN])
        theirs[UP] = left1(sides[0], UP, None, theirs[DOWN], 0)
        got_up = partner(theirs[UP])
        own1[DOWN] = left1(sides[1], DOWN, got, theirs[UP])
        far1 = {DOWN: across(own1[DOWN])}
        near1 = {DOWN: partner(own1[DOWN])}
        theirs[GATE] = left1(sides[0], GATE, None, own1[DOWN], 1)
        got_gate = partner(theirs[GATE])
        own1[UP] = left1(sides[1], UP, got_up, theirs[GATE])
        far1[UP] = across(own1[UP])
        near1[UP] = partner(own1[UP])
        own1[GATE] = left1(sides[1], GATE, got_gate, own1[UP])
        far1[GATE] = across(own1[GATE])
        near1[GATE] = partner(own1[GATE])

        last = own1[GATE]

        def optimize(which, layer, terms, where, tile, others=()):
            nonlocal last
            both = barrier((*terms, *others, last))
            terms, others = both[: len(terms)], both[len(terms) : -1]
            new[which] = adamw(terms, where, old[which], layer, tile, new[which], others)
            last = new[which][0]

        arrived = {}

        def beside(which):
            here = after(far1[which], last)
            arrived[which] = (here, partner(here))

        def first_layer(which):
            if which == DOWN:
                places = [(side * 2, 0, side * 2 + 1, 0) for side in (me, 1 - me)]
                optimize(which, 0, (near[which][0], passed[0]), places[1], 224, (near[which][1], passed[1]))
                return
            here = after(far[which], last)
            optimize(which, 0, (sums[which], here), (me, 0), 192)
            there = partner(here)
            if which == GATE:
                beside(DOWN)
            optimize(which, 0, (near[which], there), (1 - me, 0), 192)

        def places(which, of_chip):
            return [(of_chip * 2 + side, 0) if which == DOWN else (side, of_chip) for side in (me, 1 - me)]

        first_layer(DOWN)
        for which in (DOWN, UP, GATE):
            optimize(which, 1, (near1[which],), places(which, chip)[1], 224 if which == DOWN else 192)
        first_layer(UP)
        first_layer(GATE)
        for which in (DOWN, UP):
            if which == DOWN:
                beside(UP)
            (here, there), (first, second) = arrived[which], places(which, 1 - chip)
            optimize(which, 1, (here,), first + second, 224 if which == DOWN else 192, (there,))
        first, second = places(GATE, 1 - chip)
        here = after(far1[GATE], last)
        optimize(GATE, 1, (here,), first, 192)
        optimize(GATE, 1, (partner(here),), second, 192)
        return tuple(new[i][which] for which in range(3) for i in range(3))

    mapped = jax.shard_map(
        step,
        mesh=mesh,
        in_specs=(P(("rep", "dp"), None, None),) * 2 + (P(None, None, None),) * 9,
        out_specs=(P("rep", None, None),) * 9,
        check_vma=False,
    )

    def traced(*args):
        shapes = [jax.ShapeDtypeStruct(x.shape, x.dtype) for x in args]
        jax.eval_shape(mapped, *shapes)
        return mapped(*args)

    return traced
```
